32 devices in a mesh: dp: 2 (over y), row: 4 (over x, core), col: 4 (over z).
Axes of the slice: x: 2, y: 2, z: 4, core: 2. Of those that a mesh axis runs over, the one named last changes fastest.
Arguments:
- tokens: bfloat16 [2048, 8192], P(('dp', 'col'), 'row'), may hold values from -6 to 6
- frozen_weight: bfloat16 [8192, 8192], P('row', 'col'), may hold values from -0.0625 to 0.0625
- input_adapter_factor: bfloat16 [16, 8192], P(None, 'row'), may hold values from -0.0625 to 0.0625
- output_adapter_factor: bfloat16 [16, 8192], P(None, 'col'), may hold values from -1.5 to 1.5
- magnitude: float32 [8192], P('col'), may hold values from 0.5 to 2
- cotangent: bfloat16 [2048, 8192], P(('dp', 'row'), 'col'), may hold values from -6 to 6
- sequence_lengths: int32 [2, 8], P('dp'), may hold values from 1 to 512, 1024 in all within a row
Outputs:
- projected: bfloat16 [2048, 8192], P(('dp', 'row'), 'col')
- grad_mag: float32 [8192], P('col')
- input_factor_gradient: float32 [16, 8192], P(None, 'row')
- grad_b: float32 [16, 8192], P(None, 'col')
The draws below stay inside these ranges and needn't reach their ends.
Inputs may be any that keep to these rules, and one draw needn't show every extreme that they name: `sequence_lengths`: each group's 8 lengths sum to 1024, and one of them is exactly 512.
All inputs are finite; a program needn't handle non-finite values.
Results may differ from the reference program's by a relative error of at most 0.0052.
Values may be sent and summed in bfloat16 or wider, within the bound.
No kernel may reach another device: no remote copies, remote signals or barrier semaphores. Data moves between devices by JAX's collectives and lax.ppermute only.
A program may use at most 64 MiB of HBM per device.

```python
import math
import jax
import jax.numpy as jnp
import numpy as np
from jax import lax

MODEL_WIDTH = 8192
ADAPTER_RANK = 16
TOK = 1024
SEQS = 8
LONGEST = 512
GROUPS = 2
TOKENS = 2048


def levels(stream_key, dims, cuts, least, largest):
    gain = 1.0
    for position, parts in cuts:
        heights = jax.random.uniform(jax.random.fold_in(jax.random.fold_in(stream_key, 6), position), (parts,), jnp.float32, least / len(cuts), largest / len(cuts))
        gain = gain * jnp.repeat(jnp.exp(heights), dims[position] // parts).reshape((-1,) + (1,) * (len(dims) - 1 - position))
    return gain


def length_profile(count, total, reach, lean):
    weights = [(1 << 20) // math.isqrt(rank ** lean) + 1 for rank in range(2, count + 1)]
    rest, holding = total - reach - (count - 1), [1] * (count - 1)
    while rest > 0:
        free = [i for i in range(count - 1) if holding[i] < reach]
        mass, left = sum([weights[i] for i in free]), rest
        for i in free:
            extra = min(reach - holding[i], max(1, left * weights[i] // mass), rest)
            holding[i] = holding[i] + extra
            rest = rest - extra
    return np.array([reach] + holding)


def uneven(rng, amount, total, limit, skew):
    if amount == 2:
        one = jax.random.randint(rng, (), max(1, total - limit), min(limit, total - 1) + 1)
        return jnp.stack([one, total - one])
    sizes = jnp.asarray(length_profile(amount, total, limit, skew), jnp.int32)
    couples = (amount - 1) // 2
    donor, sink = sizes[1:1 + 2 * couples:2], sizes[2:2 + 2 * couples:2]
    slack = jnp.minimum(donor - 1, limit - sink)
    shifted = jax.random.randint(jax.random.fold_in(rng, 1), (couples,), 0, 1 << 20) % (slack + 1)
    sizes = sizes.at[1:1 + 2 * couples:2].set(donor - shifted).at[2:2 + 2 * couples:2].set(sink + shifted)
    return sizes[jax.random.permutation(jax.random.fold_in(rng, 2), amount)]


def centred(own_key, shape, deviation, bound, pieces=(), held_as=jnp.bfloat16):
    gain = levels(own_key, shape, pieces, -0.22, 0.18) if pieces else 1.0
    result = jax.random.normal(own_key, shape, jnp.float32) * deviation * gain
    return jnp.minimum(jnp.maximum(result, -bound), bound).astype(held_as)


def setup_inputs(seed: int = 0) -> dict:
    keys = jax.random.split(jax.random.key(seed), 8)
    tokens = centred(keys[0], (TOKENS, MODEL_WIDTH), 1.0, 6.0, ((0, 8), (1, 4)))
    frozen_weight = centred(keys[1], (MODEL_WIDTH, MODEL_WIDTH), MODEL_WIDTH ** -0.5, 0.0625, ((0, 4), (1, 4)))
    input_adapter_factor = centred(keys[2], (ADAPTER_RANK, MODEL_WIDTH), MODEL_WIDTH ** -0.5, 0.0625, ((1, 4),))
    output_adapter_factor = centred(keys[3], (ADAPTER_RANK, MODEL_WIDTH), ADAPTER_RANK ** -0.5, 1.5, ((1, 4),))
    magnitude = jnp.clip(jnp.exp(math.log(2.0) - 1.3862944 * jax.random.uniform(keys[4], (MODEL_WIDTH,), jnp.float32) ** levels(keys[4], (MODEL_WIDTH,), ((0, 4),), -0.2, 0.2)), 0.5, 2.0)
    cotangent = centred(keys[5], (TOKENS, MODEL_WIDTH), 1.0, 6.0, ((0, 8), (1, 4)))
    sequence_lengths = jax.vmap(lambda own: uneven(own, SEQS, TOK, LONGEST, 2))(jax.random.split(keys[6], GROUPS)).reshape((GROUPS, SEQS)).astype(jnp.int32)
    return dict(tokens=tokens, frozen_weight=frozen_weight, input_adapter_factor=input_adapter_factor, output_adapter_factor=output_adapter_factor, magnitude=magnitude, cotangent=cotangent, sequence_lengths=sequence_lengths)


norm_eps = 1e-06
highest_precision = lax.Precision.HIGHEST

def contract_product(left, right, left_dim, right_dim):
    return lax.dot_general(left, right, (((left_dim,), (right_dim,)), ((), ())), preferred_element_type=jnp.float32)

def token_weights(lengths, positions):
    ends = jnp.cumsum(lengths, dtype=jnp.int32)
    starts = ends - lengths
    inside = (positions[:, None] >= starts[None, :]) & (positions[:, None] < ends[None, :])
    inverse = 1.0 / lengths.astype(jnp.float32)
    return lax.optimization_barrier(jnp.sum(jnp.where(inside, inverse[None, :], jnp.float32(0.0)), axis=1))

def reference(tokens, frozen_weight, input_adapter_factor, output_adapter_factor, magnitude, cotangent, sequence_lengths):
    low_rank_update = contract_product(input_adapter_factor, output_adapter_factor, 0, 0)
    merged = frozen_weight.astype(jnp.float32) + low_rank_update
    col_norm = jnp.sqrt(lax.optimization_barrier(jnp.sum(merged * merged, axis=0)) + norm_eps)
    col_scale = magnitude / col_norm
    down_activations = contract_product(tokens, input_adapter_factor, 1, 1).astype(jnp.bfloat16)
    query_projection = jnp.dot(tokens, frozen_weight, preferred_element_type=jnp.float32) + jnp.dot(down_activations, output_adapter_factor, preferred_element_type=jnp.float32)
    projected = (query_projection * col_scale[None, :]).astype(jnp.bfloat16)
    positions = jnp.arange(TOK, dtype=jnp.int32)
    weights = jax.vmap(lambda lengths: token_weights(lengths, positions))(sequence_lengths).reshape(-1)
    grad_out = cotangent.astype(jnp.float32) * weights[:, None]
    scale_grad = lax.optimization_barrier(jnp.sum(grad_out * query_projection, axis=0))
    grad_mag = scale_grad / col_norm
    norm_coefficient = -scale_grad * magnitude / (col_norm * col_norm * col_norm)
    projection_gradient = (grad_out * col_scale[None, :]).astype(jnp.bfloat16)
    gram_product_matrix = contract_product(input_adapter_factor, input_adapter_factor, 1, 1)
    merged_input_factor = jnp.dot(input_adapter_factor, frozen_weight, preferred_element_type=jnp.float32) + jnp.dot(gram_product_matrix, output_adapter_factor.astype(jnp.float32), precision=highest_precision)
    grad_b = contract_product(down_activations, projection_gradient, 0, 0) + merged_input_factor * norm_coefficient[None, :]
    backward_rows = contract_product(projection_gradient, output_adapter_factor, 1, 1).astype(jnp.bfloat16)
    scaled_output_factor = (output_adapter_factor.astype(jnp.float32) * norm_coefficient[None, :]).astype(jnp.bfloat16)
    input_factor_gradient = contract_product(backward_rows, tokens, 0, 0) + contract_product(scaled_output_factor, frozen_weight, 1, 1)
    input_factor_gradient = input_factor_gradient + jnp.dot(contract_product(scaled_output_factor, output_adapter_factor, 1, 1), input_adapter_factor.astype(jnp.float32), precision=highest_precision)
    return (projected, grad_mag, input_factor_gradient, grad_b)
```

```python
import jax
import jax.numpy as jnp
from jax import lax
from jax.sharding import PartitionSpec as P

norm_eps = 1e-06
highest_precision = lax.Precision.HIGHEST
chunk_rows = 64
lane_count = 128


def contract_product(left, right, left_dim, right_dim):
    return lax.dot_general(
        left, right, (((left_dim,), (right_dim,)), ((), ())), preferred_element_type=jnp.float32
    )


def xor_pairs(size, bit):
    return [(i, i ^ bit) for i in range(size)]


def exchange(value, axis, bit):
    return lax.ppermute(value, axis, xor_pairs(lax.axis_size(axis), bit))


def all_sum(value, axis):
    bit = 1
    while bit < lax.axis_size(axis):
        value = value + exchange(value, axis, bit)
        bit *= 2
    return value


def chain_gather(piece):
    count = lax.axis_size("col")
    place = lax.axis_index("col")
    from_left, from_right = [piece], [piece]
    for step in range(1, count):
        right = [(i, i + 1) for i in range(step - 1, count - 1)]
        left = [(i, i - 1) for i in range(1, count - step + 1)]
        from_left.append(lax.ppermute(from_left[-1], "col", right))
        from_right.append(lax.ppermute(from_right[-1], "col", left))
    blocks = [piece]
    for step in range(1, count):
        blocks.append(jnp.where(place >= step, from_left[step], from_right[count - step]))
    return blocks


def per_device(
    tokens,
    frozen_weight,
    input_adapter_factor,
    output_adapter_factor,
    magnitude,
    cotangent,
    sequence_lengths,
):
    row_count = lax.axis_size("row")
    col_count = lax.axis_size("col")
    row_index = lax.axis_index("row")
    col_index = lax.axis_index("col")
    local_rows, features = tokens.shape
    columns = frozen_weight.shape[1]
    rank = input_adapter_factor.shape[0]
    group_rows = local_rows * col_count
    block_rows = group_rows // row_count
    per_slot = col_count // row_count
    pieces = max(1, local_rows // chunk_rows)
    piece_rows = local_rows // pieces
    slot_rows = per_slot * piece_rows

    gathered = [
        chain_gather(tokens[k * piece_rows : (k + 1) * piece_rows]) for k in range(pieces)
    ]

    low_rank_update = contract_product(input_adapter_factor, output_adapter_factor, 0, 0)
    merged = frozen_weight.astype(jnp.float32) + low_rank_update
    norm_terms = jnp.sum(merged * merged, axis=0)
    gram_partial_terms = contract_product(input_adapter_factor, input_adapter_factor, 1, 1)
    merged_factor_terms = jnp.dot(
        input_adapter_factor, frozen_weight, preferred_element_type=jnp.float32
    ) + jnp.dot(
        gram_partial_terms, output_adapter_factor.astype(jnp.float32), precision=highest_precision
    )
    norm_sq = all_sum(norm_terms[None, :], "row")[0]
    merged_input_factor = all_sum(merged_factor_terms, "row")
    col_norm = jnp.sqrt(norm_sq + norm_eps)
    col_scale = magnitude / col_norm

    lengths = sequence_lengths[0]
    ends = jnp.cumsum(lengths, dtype=jnp.int32)
    starts = ends - lengths
    positions = row_index * block_rows + jnp.arange(block_rows, dtype=jnp.int32)
    inside = (positions[:, None] >= starts[None, :]) & (positions[:, None] < ends[None, :])
    inverse = 1.0 / lengths.astype(jnp.float32)
    weights = jnp.sum(jnp.where(inside, inverse[None, :], jnp.float32(0.0)), axis=1)
    grad_out = cotangent.astype(jnp.float32) * weights[:, None]
    projection_gradient = (grad_out * col_scale[None, :]).astype(jnp.bfloat16)
    backward = contract_product(output_adapter_factor, projection_gradient, 1, 1).astype(
        jnp.bfloat16
    )
    backward = backward[None]
    bit = 1
    while bit < row_count:
        backward = jnp.concatenate([backward, exchange(backward, "row", bit)], axis=0)
        bit *= 2
    backward = backward.reshape(row_count, rank, per_slot, pieces, piece_rows)

    adapter_columns = jnp.zeros((features, lane_count), jnp.bfloat16)
    adapter_columns = lax.dynamic_update_slice(adapter_columns, input_adapter_factor.T, (0, 0))
    wide_weight = jnp.concatenate([frozen_weight, adapter_columns], axis=1)
    out_grad = grad_out.reshape(per_slot, pieces, piece_rows, columns)
    scale_terms = jnp.zeros((columns,), jnp.float32)
    row_term = jnp.zeros((rank, features), jnp.float32)
    outputs, downs = [], []
    for k in range(pieces):
        stack = jnp.zeros((group_rows // pieces, features), jnp.bfloat16)
        for step in range(col_count):
            block = (col_index - step) % col_count
            slot = ((block // per_slot) ^ row_index) * per_slot + block % per_slot
            stack = lax.dynamic_update_slice(stack, gathered[k][step], (slot * piece_rows, 0))
        partial = jnp.dot(stack, wide_weight, preferred_element_type=jnp.float32)
        parts = [partial[s * slot_rows : (s + 1) * slot_rows] for s in range(row_count)]
        bit = 1
        while bit < row_count:
            send = jnp.concatenate([p.astype(jnp.bfloat16) for p in parts[1::2]], axis=0)
            received = exchange(send, "row", bit)
            parts = [
                p + received[i * slot_rows : (i + 1) * slot_rows].astype(jnp.float32)
                for i, p in enumerate(parts[0::2])
            ]
            bit *= 2
        down = parts[0][:, columns : columns + rank].astype(jnp.bfloat16)
        projection = parts[0][:, :columns] + jnp.dot(
            down, output_adapter_factor, preferred_element_type=jnp.float32
        )
        outputs.append((projection * col_scale[None, :]).astype(jnp.bfloat16))
        downs.append(down)
        here = out_grad[:, k].reshape(slot_rows, columns)
        scale_terms = scale_terms + jnp.sum(here * projection, axis=0)
        rows = jnp.transpose(backward[:, :, :, k], (1, 0, 2, 3)).reshape(rank, -1)
        row_term = row_term + jnp.dot(rows, stack, preferred_element_type=jnp.float32)

    def in_order(values):
        width = values[0].shape[1]
        stacked = jnp.stack([v.reshape(per_slot, piece_rows, width) for v in values], axis=1)
        return stacked.reshape(block_rows, width)

    projected = in_order(outputs)
    down_activations = in_order(downs)
    bgrad_terms = contract_product(down_activations, projection_gradient, 0, 0)

    group_scale = all_sum(scale_terms[None, :], "row")
    group_coefficient = -group_scale * (magnitude / (col_norm * col_norm * col_norm))[None, :]
    scaled_output_factor = (
        output_adapter_factor.astype(jnp.float32) * group_coefficient
    ).astype(jnp.bfloat16)
    norm_term = contract_product(scaled_output_factor, frozen_weight, 1, 1) + jnp.dot(
        contract_product(scaled_output_factor, output_adapter_factor, 1, 1),
        input_adapter_factor.astype(jnp.float32),
        precision=highest_precision,
    )
    input_factor_gradient = all_sum(all_sum(row_term + norm_term, "dp"), "col")

    scale_grad = all_sum(group_scale, "dp")[0]
    bgrad_data = all_sum(all_sum(bgrad_terms, "row"), "dp")
    grad_mag = scale_grad / col_norm
    norm_coefficient = -scale_grad * magnitude / (col_norm * col_norm * col_norm)
    grad_b = bgrad_data + merged_input_factor * norm_coefficient[None, :]
    return (projected, grad_mag, input_factor_gradient, grad_b)


def solution(mesh):
    in_specs = (
        P(("dp", "col"), "row"),
        P("row", "col"),
        P(None, "row"),
        P(None, "col"),
        P("col"),
        P(("dp", "row"), "col"),
        P("dp", None),
    )
    out_specs = (P(("dp", "row"), "col"), P("col"), P(None, "row"), P(None, "col"))
    return jax.shard_map(
        per_device, mesh=mesh, in_specs=in_specs, out_specs=out_specs, check_vma=False
    )
```

```python
import functools

import jax
import jax.numpy as jnp
from jax import lax
from jax.experimental import pallas as pl
from jax.experimental.pallas import tpu as pltpu
from jax.sharding import PartitionSpec as P

norm_eps = 1e-06
highest_precision = lax.Precision.HIGHEST
chunk_rows = 128
column_tile = 1024
kernel_memory = 28 << 20


def contract_product(left, right, left_dim, right_dim):
    return lax.dot_general(
        left, right, (((left_dim,), (right_dim,)), ((), ())), preferred_element_type=jnp.float32
    )


def exchange(value, axis, bit):
    pairs = [(i, i ^ bit) for i in range(lax.axis_size(axis))]
    return lax.ppermute(value, axis, pairs)


def bits_of(axis):
    bits = []
    while (1 << len(bits)) < lax.axis_size(axis):
        bits.append(1 << len(bits))
    return bits


def all_sum(value, axis):
    for bit in bits_of(axis):
        value = value + exchange(value, axis, bit)
    return value


def all_sum_narrow(value, axis):
    for bit in bits_of(axis):
        mine = value.astype(jnp.bfloat16)
        other = exchange(mine, axis, bit)
        value = mine.astype(jnp.float32) + other.astype(jnp.float32)
    return value


def reversed_bits(value, count):
    result, size = 0, count
    while size > 1:
        result = result * 2 + (value & 1)
        value = value >> 1
        size //= 2
    return result


def prepare_kernel(weight_ref, down_ref, up_ref, norm_ref, merged_ref, gram_ref):
    features = weight_ref.shape[0]
    down = down_ref[...]
    up = up_ref[...]

    @pl.when(pl.program_id(0) == 0)
    def _():
        gram_ref[...] = contract_product(down, down, 1, 1)

    merged_ref[...] = jnp.dot(
        down, weight_ref[...], preferred_element_type=jnp.float32
    ) + jnp.dot(
        gram_ref[...],
        up.astype(jnp.float32),
        precision=highest_precision,
        preferred_element_type=jnp.float32,
    )
    step = min(256, features)
    total = jnp.zeros((1, up.shape[1]), jnp.float32)
    for start in range(0, features, step):
        merged = weight_ref[start : start + step, :].astype(jnp.float32) + contract_product(
            down[:, start : start + step], up, 0, 0
        )
        total = total + jnp.sum(merged * merged, axis=0, keepdims=True)
    norm_ref[...] = total


def prepare(weight, down, up):
    features, columns = weight.shape
    rank = down.shape[0]
    tile = min(column_tile, columns)
    return pl.pallas_call(
        prepare_kernel,
        grid=(columns // tile,),
        in_specs=[
            pl.BlockSpec((features, tile), lambda j: (0, j)),
            pl.BlockSpec((rank, features), lambda j: (0, 0)),
            pl.BlockSpec((rank, tile), lambda j: (0, j)),
        ],
        out_specs=[
            pl.BlockSpec((1, tile), lambda j: (0, j)),
            pl.BlockSpec((rank, tile), lambda j: (0, j)),
        ],
        out_shape=[
            jax.ShapeDtypeStruct((1, columns), jnp.float32),
            jax.ShapeDtypeStruct((rank, columns), jnp.float32),
        ],
        scratch_shapes=[pltpu.VMEM((rank, rank), jnp.float32)],
        cost_estimate=pl.CostEstimate(
            flops=6_000_000_000, bytes_accessed=2 * features * columns, transcendentals=0
        ),
        compiler_params=pltpu.CompilerParams(vmem_limit_bytes=kernel_memory),
        name="prepare",
    )(weight, down, up)


def block_kernel(at, choices, parts, first, *refs):
    entry, piece_index, pieces = at
    refs = list(refs)
    place_ref, length_ref = refs.pop(0), refs.pop(0)
    sources = [[refs.pop(0) for _ in range(parts)] for _ in range(choices)]
    weight_ref, down_ref, up_ref, scale_ref = (refs.pop(0) for _ in range(4))
    cotangents = [refs.pop(0) for _ in range(parts)]
    if not first:
        scale_in, grad_in, row_in = (refs.pop(0) for _ in range(3))
        del refs[:parts]
    partials = [refs.pop(0) for _ in range(parts)]
    scale_out, grad_out, row_out = (refs.pop(0) for _ in range(3))
    rows_ref, share_ref, acts_ref, acts_t_ref, back_ref, sem = refs
    step = pl.program_id(0)
    count = sources[0][0].shape[0]

    @pl.when(step == 0)
    def _():
        for c in range(choices):

            @pl.when(place_ref[entry + 1] == c)
            def _(c=c):
                for p in range(parts):
                    copy = pltpu.make_async_copy(
                        sources[c][p], rows_ref.at[pl.ds(p * count, count)], sem
                    )
                    copy.start()
                    copy.wait()

        base = (place_ref[entry + 2] * pieces + piece_index) * count
        position = base + lax.broadcasted_iota(jnp.int32, share_ref.shape, 0)
        length = jnp.zeros(share_ref.shape, jnp.int32)
        end = jnp.int32(0)
        for q in range(length_ref.shape[0]):
            start, end = end, end + length_ref[q]
            inside = (position >= start) & (position < end)
            length = jnp.where(inside, length_ref[q], length)
        share_ref[...] = 1.0 / length.astype(jnp.float32)
        rows = rows_ref[...]
        acts_ref[...] = contract_product(rows, down_ref[...], 1, 1).astype(jnp.bfloat16)
        acts_t_ref[...] = contract_product(down_ref[...], rows, 1, 1).astype(jnp.bfloat16)
        back_ref[...] = jnp.zeros_like(back_ref)

    up = up_ref[...]
    partial = jnp.dot(
        rows_ref[...], weight_ref[...], preferred_element_type=jnp.float32
    ) + jnp.dot(acts_ref[...], up, preferred_element_type=jnp.float32)
    scale = scale_ref[...]
    scale_sum = jnp.zeros_like(scale_out) if first else scale_in[...]
    grads = []
    for p in range(parts):
        piece = partial[p * count : (p + 1) * count]
        weighted = cotangents[p][0].astype(jnp.float32) * share_ref[p * count : (p + 1) * count]
        scale_sum = scale_sum + jnp.sum(weighted * piece, axis=0, keepdims=True)
        grads.append((weighted * scale).astype(jnp.bfloat16))
        partials[p][0] = piece.astype(jnp.bfloat16)
    scale_out[...] = scale_sum
    grad = grads[0] if parts == 1 else jnp.concatenate(grads, axis=0)
    grad_sum = jnp.dot(acts_t_ref[...], grad, preferred_element_type=jnp.float32)
    grad_out[...] = grad_sum if first else grad_in[...] + grad_sum
    back_ref[...] += contract_product(up, grad, 1, 1)

    @pl.when(step == pl.num_programs(0) - 1)
    def _():
        row_sum = jnp.dot(
            back_ref[...].astype(jnp.bfloat16),
            rows_ref[...],
            preferred_element_type=jnp.float32,
        )
        row_out[...] = row_sum if first else row_in[...] + row_sum


def block_step(at, scalars, sources, weight, down, up, scale, cotangents, sums):
    features, columns = weight.shape
    rank = down.shape[0]
    parts = len(cotangents)
    slots, count, _ = cotangents[0].shape
    tile = min(column_tile, columns)
    first = sums is None
    choices = len(sources)
    rows = parts * count
    moving = pl.BlockSpec((1, count, tile), lambda j, place, _: (place[at[0]], 0, j))
    wide = pl.BlockSpec((rank, tile), lambda j, *_: (0, j))
    line = pl.BlockSpec((1, tile), lambda j, *_: (0, j))
    whole = pl.BlockSpec((rank, features), lambda j, *_: (0, 0))
    in_specs = [pl.BlockSpec(memory_space=pl.ANY)] * (choices * parts)
    in_specs += [pl.BlockSpec((features, tile), lambda j, *_: (0, j)), whole, wide, line]
    in_specs += [moving] * parts
    operands = [piece for source in sources for piece in source]
    operands += [weight, down, up, scale, *cotangents]
    aliases = {}
    if not first:
        base = len(scalars) + len(operands)
        in_specs += [line, wide, whole] + [pl.BlockSpec(memory_space=pl.ANY)] * parts
        operands += [*sums[1:], *sums[0]]
        aliases = {base: parts, base + 1: parts + 1, base + 2: parts + 2}
        aliases.update({base + 3 + p: p for p in range(parts)})
    results = pl.pallas_call(
        functools.partial(block_kernel, at, choices, parts, first),
        grid_spec=pltpu.PrefetchScalarGridSpec(
            num_scalar_prefetch=len(scalars),
            grid=(columns // tile,),
            in_specs=in_specs,
            out_specs=[moving] * parts + [line, wide, whole],
            scratch_shapes=[
                pltpu.VMEM((rows, features), jnp.bfloat16),
                pltpu.VMEM((rows, 1), jnp.float32),
                pltpu.VMEM((rows, rank), jnp.bfloat16),
                pltpu.VMEM((rank, rows), jnp.bfloat16),
                pltpu.VMEM((rank, rows), jnp.float32),
                pltpu.SemaphoreType.DMA,
            ],
        ),
        out_shape=[jax.ShapeDtypeStruct((slots, count, columns), jnp.bfloat16)] * parts
        + [
            jax.ShapeDtypeStruct((1, columns), jnp.float32),
            jax.ShapeDtypeStruct((rank, columns), jnp.float32),
            jax.ShapeDtypeStruct((rank, features), jnp.float32),
        ],
        input_output_aliases=aliases,
        cost_estimate=pl.CostEstimate(
            flops=2 * rows * features * columns,
            bytes_accessed=2 * features * columns,
            transcendentals=0,
        ),
        compiler_params=pltpu.CompilerParams(vmem_limit_bytes=kernel_memory),
    )(*scalars, *operands)
    return (results[:parts], *results[parts:])


def chain_steps(pieces):
    count = lax.axis_size("col")
    even, odd = [pieces], [pieces]
    for step in range(1, count):
        arrived = []
        for parity, source in ((0, odd), (1, even)):
            pairs = []
            for i in range(parity, count - 1, 2):
                if i >= step - 1:
                    pairs.append((i, i + 1))
                if i <= count - 1 - step:
                    pairs.append((i + 1, i))
            moved = None
            if pairs:
                moved = []
                for piece in source[-1]:
                    moved.append(lax.ppermute(piece, "col", pairs))
            arrived.append(moved)
        even.append(arrived[0])
        odd.append(arrived[1])
    return even, odd


def arrival_order(count):
    order = []
    for place in range(count):
        left = [(step, 1 - place % 2, place - step) for step in range(1, place + 1)]
        right = [(step, place % 2, place + step) for step in range(1, count - place)]
        order.append(sorted(left + right))
    return order


def per_device(
    tokens,
    frozen_weight,
    input_adapter_factor,
    output_adapter_factor,
    magnitude,
    cotangent,
    sequence_lengths,
):
    row_count = lax.axis_size("row")
    col_count = lax.axis_size("col")
    row_index = lax.axis_index("row")
    col_index = lax.axis_index("col")
    local_rows, _ = tokens.shape
    columns = frozen_weight.shape[1]
    block_rows = local_rows * col_count // row_count
    per_slot = col_count // row_count
    pieces = max(1, local_rows // chunk_rows)
    count = local_rows // pieces

    token_pieces = [tokens[k * count : (k + 1) * count] for k in range(pieces)]
    chains = chain_steps(token_pieces)

    own_cotangent = cotangent.reshape(per_slot, pieces, count, columns)
    cotangents = []
    for k in range(pieces):
        held = own_cotangent[:, k]
        for bit in reversed(bits_of("row")):
            held = jnp.concatenate([held, exchange(held, "row", bit)], axis=0)
        cotangents.append(held)

    norm_terms, merged_factor_terms = prepare(
        frozen_weight, input_adapter_factor, output_adapter_factor
    )
    norm_sq = all_sum(norm_terms, "row")
    col_norm = jnp.sqrt(norm_sq + norm_eps)
    magnitude = magnitude[None, :]
    col_scale = magnitude / col_norm

    order = arrival_order(col_count)
    choices, table = [[None]], [[[place, 0] for place in range(col_count)]]
    for step in range(1, col_count):
        arrivals = [order[place][step - 1] for place in range(col_count)]
        choices.append(sorted({arrival[:2] for arrival in arrivals}))
        table.append([[a[2], choices[-1].index(a[:2])] for a in arrivals])
    table = jnp.array(table, jnp.int32)
    here = lax.dynamic_index_in_dim(table, col_index, 1, keepdims=False)
    blocks = here[:, 0]
    slot = reversed_bits(lax.div(blocks, jnp.int32(per_slot)) ^ row_index, row_count)
    slot = slot * per_slot + lax.rem(blocks, jnp.int32(per_slot))
    places = jnp.stack([slot, here[:, 1], blocks], axis=1).reshape(-1)

    sums = None
    fixed = (frozen_weight, input_adapter_factor, output_adapter_factor, col_scale)
    for step in range(col_count):
        groups = [[k] for k in range(pieces)] if step == col_count - 1 else [list(range(pieces))]
        for group in groups:
            sources = [token_pieces if c is None else chains[c[1]][c[0]] for c in choices[step]]
            sources = [[source[k] for k in group] for source in sources]
            previous = None
            if sums is not None:
                previous = ([sums[0][k] for k in group], *sums[1:])
            result = block_step(
                (3 * step, group[0], pieces),
                (places, sequence_lengths[0]),
                sources,
                *fixed,
                [cotangents[k] for k in group],
                previous,
            )
            partials = [None] * pieces if sums is None else list(sums[0])
            for k, partial in zip(group, result[0]):
                partials[k] = partial
            sums = (partials, *result[1:])
    partials, scale_terms, bgrad_terms, row_term = sums

    outputs = []
    for k in range(pieces):
        held = partials[k]
        for bit in bits_of("row"):
            half = held.shape[0] // 2
            received = exchange(held[half:], "row", bit)
            held = held[:half].astype(jnp.float32) + received.astype(jnp.float32)
            if held.shape[0] > per_slot:
                held = held.astype(jnp.bfloat16)
        outputs.append((held.astype(jnp.float32) * col_scale).astype(jnp.bfloat16))
    projected = jnp.stack(outputs, axis=1).reshape(block_rows, columns)

    scale_grad = all_sum(all_sum(scale_terms, "row"), "dp")
    grad_mag = scale_grad / col_norm
    norm_coefficient = -scale_grad * magnitude / (col_norm * col_norm * col_norm)
    scaled_output_factor = (
        output_adapter_factor.astype(jnp.float32) * norm_coefficient
    ).astype(jnp.bfloat16)
    norm_term = contract_product(scaled_output_factor, frozen_weight, 1, 1) + jnp.dot(
        contract_product(scaled_output_factor, output_adapter_factor, 1, 1),
        input_adapter_factor.astype(jnp.float32),
        precision=highest_precision,
    )
    row_term = all_sum(row_term, "dp")
    input_factor_gradient = all_sum_narrow(row_term + norm_term, "col")

    share = 1.0 / lax.axis_size("dp")
    grad_b = bgrad_terms + merged_factor_terms * (norm_coefficient * share)
    grad_b = all_sum(all_sum(grad_b, "row"), "dp")
    return (projected, grad_mag[0], input_factor_gradient, grad_b)


def solution(mesh):
    in_specs = (
        P(("dp", "col"), "row"),
        P("row", "col"),
        P(None, "row"),
        P(None, "col"),
        P("col"),
        P(("dp", "row"), "col"),
        P("dp", None),
    )
    out_specs = (P(("dp", "row"), "col"), P("col"), P(None, "row"), P(None, "col"))

    return jax.shard_map(
        per_device, mesh=mesh, in_specs=in_specs, out_specs=out_specs, check_vma=False
    )
```
